32 devices in a mesh: parts: 2 (over y), ep: 16 (over z, x, core).
Axes of the slice: x: 2, y: 2, z: 4, core: 2. Of those that a mesh axis runs over, the one named last changes fastest.
Arguments:
- tokens: bfloat16 [512, 2048], P(('parts', 'ep')), parts along dimension 0, may hold values from -6 to 6
- gate_up: bfloat16 [4096, 16, 1536], P(('parts', 'ep')), parts along dimension 0, may hold values from -0.125 to 0.125
- down_proj: bfloat16 [1536, 16, 2048], P(('parts', 'ep')), parts along dimension 0, may hold values from -0.21875 to 0.21875
- expert_ids: int32 [512, 8], P(('parts', 'ep')), parts along dimension 0, may hold values from 0 to 15, all different within a row; in each aligned block of 16 rows (0 to 15, 16 to 31, ...) at most 16 rows name the same one
- gate_weights: float32 [512, 8], P(('parts', 'ep')), parts along dimension 0, may hold values from 0.03 to 0.6
- owner_slot: int32 [32], P('parts'), parts along dimension 0, may hold values from 0 to 15, each once
Outputs:
- moe_out: bfloat16 [512, 2048], P(('parts', 'ep')), parts along dimension 0
- channel_scale: float32 [32, 3584], P(('parts', 'ep')), parts along dimension 0
The draws below stay inside these ranges and needn't reach their ends.
There are 2 independent parts, one for each index of `parts`. The reference program is written for one: setup_inputs(seed, part) draws one part's arguments, and reference() takes and returns one part's arrays. A program takes and returns all parts, laid end to end along the dimension named above; each array names one. Nothing has to cross between parts.
Inputs may be any that keep to these rules, and one draw needn't show every extreme that they name: `expert_ids`: each row names 8 different experts; among the rows of one device no expert is named more than 16 times, a bound that some block reaches. `owner_slot`: A permutation: each slot holds exactly one expert.
All inputs are finite; a program needn't handle non-finite values.
Results may differ from the reference program's by a relative error of at most 0.0058.
Values may be sent and summed in bfloat16 or wider, within the bound.
A program may use at most 128 MiB of HBM per device.

```python
import math
import jax
import jax.numpy as jnp
import numpy as np
from jax import lax

D = 2048
F = 768
TOPK = 8
TOK_DEV = 16
EXPERTS = 16
TOKENS = 256
CAP = 16
N_EP = 16


def levels(key, dims, cuts, low, largest):
    level, own = 1.0, jax.random.fold_in(key, 6)
    for position, shards_of in cuts:
        draws = jnp.exp(jax.random.uniform(jax.random.fold_in(own, position), (shards_of,), jnp.float32, low / len(cuts), largest / len(cuts)))
        level = level * jnp.repeat(draws, dims[position] // shards_of).reshape([-1 if axis == position else 1 for axis in range(len(dims))])
    return level


def deal_out(rng, own, number, rows, number_of, top, most, slope):
    order = jax.random.permutation(rng, number_of)
    packed, common = portions_of(number_of, rows * top, most, slope, True), portions_of(number_of, rows * top, most, slope, False)
    places = jnp.arange(number_of)

    def named(sizes, offset_by):
        used = int((sizes > 0).sum())
        fixed = max(1, used // 4)
        shifted = fixed + (places - fixed + offset_by * (used - fixed)) % max(1, number_of - fixed)
        return jnp.zeros((number_of,), jnp.int32).at[order[jnp.where(places < fixed, places, shifted)]].set(jnp.asarray(sizes, jnp.int32))

    sizes = jnp.where(number % 4 == 0, named(packed, number // 4), named(common, number - number // 4 - 1))
    mixed = jax.random.permutation(jax.random.fold_in(own, 3), number_of)
    source_of, sink = mixed[0:number_of // 2 * 2:2], mixed[1:number_of // 2 * 2:2]
    slack = jnp.minimum(sizes[source_of] - 1, most - sizes[sink]) // 2
    slack = jnp.where((source_of == order[0]) | (sink == order[0]) | (sizes[sink] == 0), 0, jnp.maximum(slack, 0))
    shifted = jax.random.randint(jax.random.fold_in(own, 4), (number_of // 2,), 0, 1 << 20) % (slack + 1)
    sizes = sizes.at[source_of].add(-shifted).at[sink].add(shifted)
    members = jnp.searchsorted(jnp.cumsum(sizes), jnp.arange(rows * top), side="right").astype(jnp.int32)
    listing = members.reshape(top, rows).T
    listing = listing[jax.random.permutation(jax.random.fold_in(own, 1), rows)]
    offset_by = jax.random.randint(jax.random.fold_in(own, 2), (rows, 1), 0, top)
    return jnp.take_along_axis(listing, (jnp.arange(top)[None, :] + offset_by) % top, axis=1)


def portions_of(amount, total, limit, lean, full):
    loads = [(1 << 20) // math.isqrt(grade ** lean) + 1 for grade in range(1, amount + 1)]
    largest = limit if full else min(limit, max(-(-total // amount), total * loads[0] // sum(loads)))
    least = 1 if total - largest >= amount - 1 else 0
    given, spare = [largest] + [least] * (amount - 1), total - largest - least * (amount - 1)
    while spare > 0:
        movable = [i for i in range(1, amount) if given[i] < largest] or [i for i in range(1, amount) if given[i] < limit]
        whole, budget = sum([loads[i] for i in movable]), spare
        for i in movable:
            more = min(limit - given[i], max(1, budget * loads[i] // whole), spare)
            given[i] = given[i] + more
            spare = spare - more
    return np.array(given)


def normal_values(key, shape, scale, most, cuts=(), held_as=jnp.bfloat16):
    factor_of = levels(key, shape, cuts, -0.22, 0.18) if cuts else 1.0
    values = jax.random.normal(key, shape, jnp.float32) * scale * factor_of
    return jnp.minimum(jnp.maximum(values, -most), most).astype(held_as)


def setup_inputs(seed: int = 0, part: int = 0) -> dict:
    key_list = jax.random.split(jax.random.key(seed), 7)
    part_splits = jax.random.split(jax.random.fold_in(key_list[6], part), 7)
    tokens = normal_values(part_splits[0], (TOKENS, D), 1.0, 6.0, ((0, 16),))
    gate_up = normal_values(part_splits[1], (D, EXPERTS, 2 * F), D ** -0.5, 0.125, ((0, 16),))
    down_proj = normal_values(part_splits[2], (F, EXPERTS, D), F ** -0.5, 0.21875, ((0, 16),))
    expert_ids_keys = jax.random.split(jax.random.fold_in(part_splits[3], 1), TOKENS // TOK_DEV)
    expert_ids_turns = jax.random.permutation(jax.random.fold_in(part_splits[3], 3), TOKENS // TOK_DEV)
    expert_ids = jax.vmap(lambda own, number: deal_out(jax.random.fold_in(part_splits[3], 2), own, number, TOK_DEV, EXPERTS, TOPK, CAP, 1))(expert_ids_keys, expert_ids_turns).reshape((TOKENS, TOPK))
    gate_weights = jnp.clip(jnp.exp(math.log(0.6) - 2.9957323 * jax.random.uniform(part_splits[4], (TOKENS, TOPK), jnp.float32) ** levels(part_splits[4], (TOKENS, TOPK), ((0, 16),), -0.2, 0.2)), 0.03, 0.6)
    owner_slot = jax.random.permutation(part_splits[5], EXPERTS).astype(jnp.int32)
    return dict(tokens=tokens, gate_up=gate_up, down_proj=down_proj, expert_ids=expert_ids, gate_weights=gate_weights, owner_slot=owner_slot)


def expert_ffn(rows, w_up, w_down):
    hidden = jnp.dot(rows, w_up, preferred_element_type=jnp.float32)
    ffn_width = w_up.shape[1] // 2
    activated = (jax.nn.silu(hidden[:, :ffn_width]) * hidden[:, ffn_width:]).astype(jnp.bfloat16)
    return jnp.dot(activated, w_down, preferred_element_type=jnp.float32).astype(jnp.bfloat16)

def column_scales(gate_up, down_proj):
    gate_scale = lax.optimization_barrier(jnp.max(jnp.abs(gate_up), axis=0)).astype(jnp.float32) * math.sqrt(gate_up.shape[0])
    down_scale = lax.optimization_barrier(jnp.max(jnp.abs(down_proj), axis=0)).astype(jnp.float32) * math.sqrt(down_proj.shape[0])
    return jnp.concatenate([gate_scale, down_scale], axis=1)

def reference(tokens, gate_up, down_proj, expert_ids, gate_weights, owner_slot):
    tok_all, model_width = tokens.shape
    top_count = expert_ids.shape[1]
    experts_all = gate_up.shape[1]
    most_rows = N_EP * CAP
    flat_ids = expert_ids.reshape(-1).astype(jnp.int32)
    ordering = jnp.argsort(flat_ids, stable=True).astype(jnp.int32)
    experts_iota = jnp.arange(experts_all, dtype=jnp.int32)
    counts = lax.optimization_barrier(jnp.sum((flat_ids[:, None] == experts_iota[None, :]).astype(jnp.int32), axis=0))
    starts = (jnp.cumsum(counts) - counts).astype(jnp.int32)
    padded = jnp.concatenate([ordering, jnp.zeros((most_rows,), jnp.int32)])
    flat_gates = gate_weights.reshape(-1)

    def visit(mixed, expert):
        picked = lax.dynamic_slice_in_dim(padded, starts[expert], most_rows)
        is_live = jnp.arange(most_rows, dtype=jnp.int32) < counts[expert]
        token_row = (picked // top_count).astype(jnp.int32)
        weighting = jnp.where(is_live, flat_gates[picked], jnp.zeros_like(flat_gates[picked]))
        rows = tokens[token_row]
        w_up = lax.dynamic_index_in_dim(gate_up, expert, 1, keepdims=False)
        w_down = lax.dynamic_index_in_dim(down_proj, expert, 1, keepdims=False)
        expert_out = expert_ffn(rows, w_up, w_down)
        mixed = mixed.at[token_row].add(weighting[:, None] * expert_out.astype(jnp.float32))
        return (mixed, None)
    mixed, ignored = lax.scan(visit, jnp.zeros((tok_all, model_width), jnp.float32), experts_iota)
    scales = column_scales(gate_up, down_proj)
    inverse = jnp.zeros((experts_all,), jnp.int32).at[owner_slot].set(experts_iota)
    return (mixed.astype(jnp.bfloat16), scales[inverse])
```

```python
import functools
import math

import jax
import jax.numpy as jnp
from jax import lax
from jax.experimental import pallas as pl
from jax.experimental.pallas import tpu as pltpu
from jax.sharding import PartitionSpec as P


def expert_block(arrived, held_up, held_down):
    hidden = jnp.einsum("rjd,djf->rjf", arrived, held_up, preferred_element_type=jnp.float32)
    ffn_width = held_up.shape[2] // 2
    activated = (jax.nn.silu(hidden[..., :ffn_width]) * hidden[..., ffn_width:]).astype(
        jnp.bfloat16
    )
    return jnp.einsum(
        "rjf,fjd->rjd", activated, held_down, preferred_element_type=jnp.float32
    ).astype(jnp.bfloat16)


def column_scales(gate_up, down_proj):
    gate_scale = jnp.max(jnp.abs(gate_up), axis=0).astype(jnp.float32) * math.sqrt(gate_up.shape[0])
    down_scale = jnp.max(jnp.abs(down_proj), axis=0).astype(jnp.float32) * math.sqrt(
        down_proj.shape[0]
    )
    return jnp.concatenate([gate_scale, down_scale], axis=1)


def shards(tokens, gate_up, down_proj, expert_ids, gate_weights, owner_slot):
    tok_rows, model_width = tokens.shape
    top_count = expert_ids.shape[1]
    slots_all = gate_up.shape[1]
    devices = lax.axis_size("ep")
    own_count = slots_all // devices
    capacity = 2 * tok_rows * top_count // slots_all
    experts_iota = jnp.arange(slots_all, dtype=jnp.int32)
    inverse = jnp.zeros((slots_all,), jnp.int32).at[owner_slot].set(experts_iota)
    flat_ids = expert_ids.reshape(-1)
    one_hot = (flat_ids[:, None] == experts_iota[None, :]).astype(jnp.int32)
    slot_rank = jnp.sum((jnp.cumsum(one_hot, axis=0) - 1) * one_hot, axis=1)
    position = slot_rank * slots_all + flat_ids
    source_rows = jnp.repeat(tokens, top_count, axis=0)
    outbox = (
        jnp.zeros((capacity * slots_all, model_width), jnp.bfloat16).at[position].set(source_rows)
    )
    outbox = outbox.reshape(capacity, slots_all, model_width)
    held_up, held_down = (
        lax.all_to_all(gate_up, "ep", split_axis=1, concat_axis=0, tiled=True),
        lax.all_to_all(down_proj, "ep", split_axis=1, concat_axis=0, tiled=True),
    )
    arrived = lax.all_to_all(outbox, "ep", split_axis=1, concat_axis=0, tiled=True)
    expert_out = expert_block(arrived, held_up, held_down)
    returned = lax.all_to_all(expert_out, "ep", split_axis=0, concat_axis=1, tiled=True).reshape(
        capacity * slots_all, model_width
    )
    picked = returned[position].astype(jnp.float32).reshape(tok_rows, top_count, model_width)
    moe_out = jnp.sum(picked * gate_weights[:, :, None], axis=1).astype(jnp.bfloat16)
    scales = column_scales(held_up, held_down)
    every_row = lax.all_gather(scales, "ep", axis=0, tiled=True)
    mine = lax.dynamic_slice_in_dim(inverse, lax.axis_index("ep") * own_count, own_count)
    scales = jnp.take(every_row, mine, axis=0)
    return (moe_out, scales)


MESH = pl.DeviceIdType.MESH
F32, BF16 = jnp.float32, jnp.bfloat16


def fused_kernel(
    dims, tok_ref, meta_ref, slot_ref, up_hbm, down_hbm, out_ref, scale_ref,
    w_ref, wt_ref, d_ref, tok_all, tok_t, meta_all, meta_t, x_ref, h_ref, act_ref, a_ref,
    o_ref, s_send, s_recv, *rest,
):
    n, bits, top, out_chunks = dims
    hs, hr = rest[:bits], rest[bits : 2 * bits]
    os_, or_ = rest[2 * bits : 3 * bits], rest[3 * bits : 4 * bits]
    load_sem, small_send, small_recv, h_ssem, h_rsem, o_ssem, o_rsem = rest[4 * bits :]
    me = lax.axis_index("ep")
    own = tok_ref.shape[0]
    total = tok_all.shape[0]
    depth = tok_all.shape[1]
    experts = slot_ref.shape[1]
    half = w_ref.shape[1] // 2
    fl = half // n
    width = d_ref.shape[1]
    root_d, root_f = math.sqrt(depth * n), math.sqrt(fl * n)

    load_w = pltpu.make_async_copy(up_hbm, w_ref, load_sem.at[0])
    load_d = pltpu.make_async_copy(down_hbm, d_ref, load_sem.at[1])
    load_w.start()
    load_d.start()

    barrier = pltpu.get_barrier_semaphore()
    for i in range(1, n):
        pl.semaphore_signal(
            barrier, inc=1, device_id={"ep": lax.rem(me + i, n)}, device_id_type=MESH
        )
    pl.semaphore_wait(barrier, n - 1)

    def remote(src, dst, ssem, rsem, peer):
        return pltpu.make_async_remote_copy(
            src_ref=src, dst_ref=dst, send_sem=ssem, recv_sem=rsem,
            device_id={"ep": peer}, device_id_type=MESH,
        )

    mine = pl.ds(pl.multiple_of(me * own, own), own)

    def tok_copy(i):
        peer = lax.rem(me + i, n)
        cols = pl.ds(pl.multiple_of(peer * depth, depth), depth)
        return remote(
            tok_ref.at[:, cols], tok_all.at[mine, :], small_send.at[0, i], small_recv.at[0, i], peer
        )

    def meta_copy(i):
        peer = lax.rem(me + i, n)
        return remote(
            meta_ref, meta_all.at[mine, :], small_send.at[1, i], small_recv.at[1, i], peer
        )

    def scale_copy(i):
        peer = lax.rem(me + i, n)
        return remote(
            s_send.at[peer], s_recv.at[me], small_send.at[2, i], small_recv.at[2, i], peer
        )

    for i in range(1, n):
        meta_copy(i).start()
        tok_copy(i).start()
    tok_all[mine, :] = tok_ref[:, pl.ds(pl.multiple_of(me * depth, depth), depth)]
    meta_all[mine, :] = meta_ref[...]
    a_ref[...] = jnp.zeros_like(a_ref)

    load_w.wait()
    tile = 2 * depth

    @pl.loop(0, w_ref.shape[1] // tile)
    def _(c):
        cols = pl.ds(pl.multiple_of(c * tile, tile), tile)

        @pl.loop(0, w_ref.shape[0] // tile)
        def _(r):
            rows = pl.ds(pl.multiple_of(r * tile, tile), tile)
            wt_ref[cols, rows] = w_ref[rows, cols].T

    for i in range(1, n):
        meta_copy(i).wait_recv()
        tok_copy(i).wait_recv()
    tok_t[...] = tok_all[...].astype(F32).T
    meta_t[...] = meta_all[...].T

    lanes = lax.broadcasted_iota(jnp.int32, (experts, total), 0).astype(F32)

    def mask_of(k):
        return meta_t[pl.ds(k, 1), :] == lanes

    def partner(s):
        bit = 1 << s
        return me + bit * (1 - 2 * lax.rem(me // bit, 2))

    def h_copy(k, s):
        return remote(hs[s].at[k], hr[s].at[k], h_ssem.at[s, k], h_rsem.at[s, k], partner(s))

    def o_copy(q, s):
        return remote(os_[s].at[q], or_[s].at[q], o_ssem.at[s, q], o_rsem.at[s, q], partner(s))

    def h_rows(k, j, part):
        return h_ref[k, pl.ds(pl.multiple_of(part * half + j * fl, 16), fl), :]

    def h_sum(k, j, s, part):
        total_ = h_rows(k, j, part)
        for prior in range(s):
            total_ += hr[prior][k, j // (2 << prior), pl.ds(part * fl, fl), :].astype(F32)
        return total_

    def product(k):
        mask = mask_of(k)

        @pl.loop(0, depth // 8)
        def _(block):
            for inner in range(8):
                d = block * 8 + inner
                row = jnp.where(mask, tok_t[pl.ds(d, 1), :], 0.0)
                x_ref[pl.ds(pl.multiple_of(d * experts, experts), experts), :] = row.astype(BF16)

        @pl.loop(0, wt_ref.shape[0] // tile)
        def _(r):
            rows = pl.ds(pl.multiple_of(r * tile, tile), tile)
            h_ref[k, rows, :] = jnp.dot(wt_ref[rows, :], x_ref[...], preferred_element_type=F32)

    def h_send(k, s):
        if s > 0:
            h_copy(k, s - 1).wait_recv()
        bit = 1 << s
        base = (1 - lax.rem(me // bit, 2)) * bit + lax.rem(me, bit)
        for m in range(n // (2 * bit)):
            j = m * 2 * bit + base
            for part in range(2):
                hs[s][k, m, pl.ds(part * fl, fl), :] = h_sum(k, j, s, part).astype(BF16)
        h_copy(k, s).start()

    def h_final(k):
        h_copy(k, bits - 1).wait_recv()
        gate = h_sum(k, me, bits, 0)
        act = gate / (1.0 + jnp.exp(-gate)) * h_sum(k, me, bits, 1)
        act_ref[...] = act * meta_t[pl.ds(top + k, 1), :]
        mask = mask_of(k)

        @pl.loop(0, fl // 8)
        def _(block):
            for inner in range(8):
                f = block * 8 + inner
                rows = pl.ds(pl.multiple_of(f * experts, experts), experts)
                a_ref[rows, :] += jnp.where(mask, act_ref[pl.ds(f, 1), :], 0.0)

    def scales_out():
        def up_max(r, best):
            rows = pl.ds(pl.multiple_of(r * experts, experts), experts)
            return jnp.maximum(best, jnp.abs(w_ref[rows, :]))

        def down_max(r, best):
            rows = pl.ds(pl.multiple_of(r * experts, experts), experts)
            return jnp.maximum(best, jnp.abs(d_ref[rows, :]))

        choose = (
            lax.broadcasted_iota(jnp.int32, (experts, experts), 0)
            == jnp.broadcast_to(slot_ref[...], (experts, experts))
        ).astype(F32).astype(BF16)
        best = lax.fori_loop(0, depth, up_max, jnp.zeros((experts, 2 * half), BF16))
        up = jnp.dot(choose, best, preferred_element_type=F32)
        load_d.wait()
        best = lax.fori_loop(0, fl, down_max, jnp.zeros((experts, width), BF16))
        down = jnp.dot(choose, best, preferred_element_type=F32)
        for slot in range(experts):
            s_send[slot, :, pl.ds(0, 2 * half)] = up[slot : slot + 1]
            s_send[slot, :, pl.ds(2 * half, width)] = down[slot : slot + 1]
        for i in range(1, n):
            scale_copy(i).start()
        s_recv[me] = s_send[me]

    @pl.loop(0, top + bits)
    def _(step):
        @pl.when(step < top)
        def _():
            product(step)
            h_send(step, 0)

        for s in range(1, bits):
            @pl.when((step >= s) & (step < top + s))
            def _():
                h_send(step - s, s)

        @pl.when(step >= bits)
        def _():
            h_final(step - bits)

        @pl.when(step == 0)
        def _():
            scales_out()

    cols_out = width // out_chunks
    a_t = a_ref[...].T.astype(BF16)

    def o_sum(q, j, s):
        total_ = o_ref[q, pl.ds(pl.multiple_of(j * own, own), own), :]
        for prior in range(s):
            total_ += or_[prior][q, j // (2 << prior)].astype(F32)
        return total_

    def o_send(q, s):
        if s > 0:
            o_copy(q, s - 1).wait_recv()
        bit = 1 << s
        base = (1 - lax.rem(me // bit, 2)) * bit + lax.rem(me, bit)
        for m in range(n // (2 * bit)):
            os_[s][q, m] = o_sum(q, m * 2 * bit + base, s).astype(BF16)
        o_copy(q, s).start()

    for step in range(out_chunks + bits):
        if step < out_chunks:
            o_ref[step] = jnp.dot(
                a_t, d_ref[:, pl.ds(step * cols_out, cols_out)], preferred_element_type=F32
            )
            o_send(step, 0)
        for s in range(1, bits):
            if s <= step < out_chunks + s:
                o_send(step - s, s)
        if step >= bits:
            q = step - bits
            o_copy(q, bits - 1).wait_recv()
            out_ref[:, pl.ds(q * cols_out, cols_out)] = o_sum(q, me, bits).astype(BF16)

    for i in range(1, n):
        scale_copy(i).wait_recv()
    best = s_recv[0]
    for i in range(1, n):
        best = jnp.maximum(best, s_recv[i])
    scale_ref[:, pl.ds(0, 2 * half)] = best[:, : 2 * half] * root_d
    scale_ref[:, pl.ds(2 * half, width)] = best[:, 2 * half :] * root_f
    for i in range(1, n):
        meta_copy(i).wait_send()
        tok_copy(i).wait_send()
        scale_copy(i).wait_send()

    @pl.loop(0, top)
    def _(k):
        for s in range(bits):
            h_copy(k, s).wait_send()

    for q in range(out_chunks):
        for s in range(bits):
            o_copy(q, s).wait_send()


def fused(tokens, gate_up, down_proj, expert_ids, gate_weights, owner_slot):
    n = lax.axis_size("ep")
    bits = n.bit_length() - 1
    own, width = tokens.shape
    depth, experts, both = gate_up.shape
    fl = down_proj.shape[0]
    top = expert_ids.shape[1]
    total = own * n
    out_chunks = 2
    meta = jnp.concatenate([expert_ids.astype(F32), gate_weights], axis=1)
    meta = jnp.pad(meta, ((0, 0), (0, 128 - 2 * top)))
    vmem = pl.BlockSpec(memory_space=pltpu.VMEM)
    hbm = pl.BlockSpec(memory_space=pl.ANY)
    counts = [n >> (s + 1) for s in range(bits)]
    hidden_bufs = [pltpu.VMEM((top, c, 2 * fl, total), BF16) for c in counts]
    out_bufs = [pltpu.VMEM((out_chunks, c, own, width // out_chunks), BF16) for c in counts]
    return pl.pallas_call(
        functools.partial(fused_kernel, (n, bits, top, out_chunks)),
        out_shape=(
            jax.ShapeDtypeStruct((own, width), BF16),
            jax.ShapeDtypeStruct((1, both + width), F32),
        ),
        in_specs=[vmem, vmem, vmem, hbm, hbm],
        out_specs=(vmem, vmem),
        scratch_shapes=[
            pltpu.VMEM((depth * experts, both), BF16),
            pltpu.VMEM((both, depth * experts), BF16),
            pltpu.VMEM((fl * experts, width), BF16),
            pltpu.VMEM((total, depth), BF16),
            pltpu.VMEM((depth, total), F32),
            pltpu.VMEM((total, 128), F32),
            pltpu.VMEM((128, total), F32),
            pltpu.VMEM((depth * experts, total), BF16),
            pltpu.VMEM((top, both, total), F32),
            pltpu.VMEM((fl, total), F32),
            pltpu.VMEM((fl * experts, total), F32),
            pltpu.VMEM((out_chunks, total, width // out_chunks), F32),
            pltpu.VMEM((n, 1, both + width), F32),
            pltpu.VMEM((n, 1, both + width), F32),
            *hidden_bufs, *hidden_bufs, *out_bufs, *out_bufs,
            pltpu.SemaphoreType.DMA((2,)),
            pltpu.SemaphoreType.DMA((3, n)),
            pltpu.SemaphoreType.DMA((3, n)),
            pltpu.SemaphoreType.DMA((bits, top)),
            pltpu.SemaphoreType.DMA((bits, top)),
            pltpu.SemaphoreType.DMA((bits, out_chunks)),
            pltpu.SemaphoreType.DMA((bits, out_chunks)),
        ],
        compiler_params=pltpu.CompilerParams(
            collective_id=0, has_side_effects=True, vmem_limit_bytes=60 * 2**20
        ),
    )(
        tokens,
        meta,
        owner_slot.reshape(1, experts),
        gate_up.reshape(depth * experts, both),
        down_proj.reshape(fl * experts, width),
    )


def layer(tokens, gate_up, down_proj, expert_ids, gate_weights, owner_slot):
    n = lax.axis_size("ep")
    own = tokens.shape[0]
    depth, experts, both = gate_up.shape
    partials = n * own * expert_ids.shape[1] * both
    aligned = (
        n & (n - 1) == 0 and depth % 128 == 0 and experts == n and experts % 16 == 0
        and down_proj.shape[0] % 16 == 0 and own % 16 == 0
    )
    args = (tokens, gate_up, down_proj, expert_ids, gate_weights, owner_slot)
    return fused(*args) if aligned and partials <= gate_up.size else shards(*args)


def solution(mesh):
    in_specs = (
        P(("parts", "ep"), None),
        P(("parts", "ep"), None, None),
        P(("parts", "ep"), None, None),
        P(("parts", "ep"), None),
        P(("parts", "ep"), None),
        P("parts"),
    )
    out_specs = (P(("parts", "ep"), None), P(("parts", "ep"), None))
    return jax.shard_map(layer, mesh=mesh, in_specs=in_specs, out_specs=out_specs, check_vma=False)
```

```python
import functools
import math

import jax
import jax.numpy as jnp
from jax import lax
from jax.experimental import pallas as pl
from jax.experimental.pallas import tpu as pltpu
from jax.sharding import PartitionSpec as P


def expert_block(arrived, held_up, held_down):
    hidden = jnp.einsum("rjd,djf->rjf", arrived, held_up, preferred_element_type=jnp.float32)
    ffn_width = held_up.shape[2] // 2
    activated = (jax.nn.silu(hidden[..., :ffn_width]) * hidden[..., ffn_width:]).astype(
        jnp.bfloat16
    )
    return jnp.einsum(
        "rjf,fjd->rjd", activated, held_down, preferred_element_type=jnp.float32
    ).astype(jnp.bfloat16)


def column_scales(gate_up, down_proj):
    gate_scale = jnp.max(jnp.abs(gate_up), axis=0).astype(jnp.float32) * math.sqrt(gate_up.shape[0])
    down_scale = jnp.max(jnp.abs(down_proj), axis=0).astype(jnp.float32) * math.sqrt(
        down_proj.shape[0]
    )
    return jnp.concatenate([gate_scale, down_scale], axis=1)


def shards(tokens, gate_up, down_proj, expert_ids, gate_weights, owner_slot):
    tok_rows, model_width = tokens.shape
    top_count = expert_ids.shape[1]
    slots_all = gate_up.shape[1]
    devices = lax.axis_size("ep")
    own_count = slots_all // devices
    capacity = 2 * tok_rows * top_count // slots_all
    experts_iota = jnp.arange(slots_all, dtype=jnp.int32)
    inverse = jnp.zeros((slots_all,), jnp.int32).at[owner_slot].set(experts_iota)
    flat_ids = expert_ids.reshape(-1)
    one_hot = (flat_ids[:, None] == experts_iota[None, :]).astype(jnp.int32)
    slot_rank = jnp.sum((jnp.cumsum(one_hot, axis=0) - 1) * one_hot, axis=1)
    position = slot_rank * slots_all + flat_ids
    source_rows = jnp.repeat(tokens, top_count, axis=0)
    outbox = (
        jnp.zeros((capacity * slots_all, model_width), jnp.bfloat16).at[position].set(source_rows)
    )
    outbox = outbox.reshape(capacity, slots_all, model_width)
    held_up, held_down = (
        lax.all_to_all(gate_up, "ep", split_axis=1, concat_axis=0, tiled=True),
        lax.all_to_all(down_proj, "ep", split_axis=1, concat_axis=0, tiled=True),
    )
    arrived = lax.all_to_all(outbox, "ep", split_axis=1, concat_axis=0, tiled=True)
    expert_out = expert_block(arrived, held_up, held_down)
    returned = lax.all_to_all(expert_out, "ep", split_axis=0, concat_axis=1, tiled=True).reshape(
        capacity * slots_all, model_width
    )
    picked = returned[position].astype(jnp.float32).reshape(tok_rows, top_count, model_width)
    moe_out = jnp.sum(picked * gate_weights[:, :, None], axis=1).astype(jnp.bfloat16)
    scales = column_scales(held_up, held_down)
    every_row = lax.all_gather(scales, "ep", axis=0, tiled=True)
    mine = lax.dynamic_slice_in_dim(inverse, lax.axis_index("ep") * own_count, own_count)
    scales = jnp.take(every_row, mine, axis=0)
    return (moe_out, scales)


MESH = pl.DeviceIdType.MESH
F32, BF16 = jnp.float32, jnp.bfloat16


def fused_kernel(
    dims, tok_ref, ids_ref, gate_ref, slot_ref, up_hbm, down_hbm, out_ref, scale_ref,
    w_ref, wt_ref, d_ref, meta32, meta_ref, tok_all, tok_t, meta_all, id_row, gate_row, x_ref,
    h_ref, act_ref, a_ref, o_ref, out32, s_send, s_recv, *rest,
):
    n, bits, chunks, groups = dims
    hs, hr = rest[:bits], rest[bits : 2 * bits]
    os_, or_ = rest[2 * bits : 3 * bits], rest[3 * bits : 4 * bits]
    load_sem, small_send, small_recv, h_ssem, h_rsem, o_ssem, o_rsem = rest[4 * bits :]
    me = lax.axis_index("ep")
    own = tok_ref.shape[0]
    total = tok_all.shape[0]
    depth = tok_all.shape[1]
    experts = slot_ref.shape[1]
    top = ids_ref.shape[1]
    per = chunks // groups
    span = total // groups
    copies = total // span
    small = own // groups
    half = w_ref.shape[1] // 2
    fl = half // n
    width = d_ref.shape[1]
    root_d, root_f = math.sqrt(depth * n), math.sqrt(fl * n)

    load_w = pltpu.make_async_copy(up_hbm, w_ref, load_sem.at[0])
    load_d = pltpu.make_async_copy(down_hbm, d_ref, load_sem.at[1])
    load_w.start()
    load_d.start()

    meta32[...] = jnp.zeros_like(meta32)
    gates = gate_ref[...]
    meta32[:, 0:top] = ids_ref[...].astype(F32)
    for piece in range(1, 4):
        high = gates.astype(BF16).astype(F32)
        meta32[:, piece * top : (piece + 1) * top] = high
        gates = gates - high
    meta_ref[...] = meta32[...].astype(BF16)

    barrier = pltpu.get_barrier_semaphore()
    for i in range(1, n):
        pl.semaphore_signal(
            barrier, inc=1, device_id={"ep": lax.rem(me + i, n)}, device_id_type=MESH
        )
    pl.semaphore_wait(barrier, n - 1)

    def remote(src, dst, ssem, rsem, peer):
        return pltpu.make_async_remote_copy(
            src_ref=src, dst_ref=dst, send_sem=ssem, recv_sem=rsem,
            device_id={"ep": peer}, device_id_type=MESH,
        )

    mine = pl.ds(pl.multiple_of(me * own, own), own)

    def tok_copy(i):
        peer = lax.rem(me + i, n)
        cols = pl.ds(pl.multiple_of(peer * depth, depth), depth)
        return remote(
            tok_ref.at[:, cols], tok_all.at[mine, :], small_send.at[0, i], small_recv.at[0, i], peer
        )

    def meta_copy(i):
        peer = lax.rem(me + i, n)
        return remote(
            meta_ref, meta_all.at[mine, :], small_send.at[1, i], small_recv.at[1, i], peer
        )

    def scale_copy(i):
        peer = lax.rem(me + i, n)
        return remote(
            s_send.at[peer], s_recv.at[me], small_send.at[2, i], small_recv.at[2, i], peer
        )

    for i in range(1, n):
        meta_copy(i).start()
        tok_copy(i).start()
    tok_all[mine, :] = tok_ref[:, pl.ds(pl.multiple_of(me * depth, depth), depth)]
    meta_all[mine, :] = meta_ref[...]
    a_ref[...] = jnp.zeros_like(a_ref)

    def scales_in():
        def up_max(r, best):
            rows = pl.ds(pl.multiple_of(r * experts, experts), experts)
            return jnp.maximum(best, jnp.abs(w_ref[rows, :]))

        def down_max(r, best):
            rows = pl.ds(pl.multiple_of(r * experts, experts), experts)
            return jnp.maximum(best, jnp.abs(d_ref[rows, :]))

        choose = (
            lax.broadcasted_iota(jnp.int32, (experts, experts), 0)
            == jnp.broadcast_to(slot_ref[...], (experts, experts))
        ).astype(F32).astype(BF16)
        best = lax.fori_loop(0, depth, up_max, jnp.zeros((experts, 2 * half), BF16))
        up = jnp.dot(choose, best, preferred_element_type=F32)
        load_d.wait()
        best = lax.fori_loop(0, fl, down_max, jnp.zeros((experts, width), BF16))
        down = jnp.dot(choose, best, preferred_element_type=F32)
        for slot in range(experts):
            s_send[slot, :, pl.ds(0, 2 * half)] = up[slot : slot + 1]
            s_send[slot, :, pl.ds(2 * half, width)] = down[slot : slot + 1]
        s_recv[me] = s_send[me]

    load_w.wait()
    tile = 2 * depth

    @pl.loop(0, w_ref.shape[1] // tile)
    def _(c):
        cols = pl.ds(pl.multiple_of(c * tile, tile), tile)

        @pl.loop(0, w_ref.shape[0] // tile)
        def _(r):
            rows = pl.ds(pl.multiple_of(r * tile, tile), tile)
            wt_ref[cols, rows] = w_ref[rows, cols].T

    scales_in()
    for i in range(1, n):
        meta_copy(i).wait_recv()
        tok_copy(i).wait_recv()

    row = lax.broadcasted_iota(jnp.int32, (total, total), 0)
    col = lax.broadcasted_iota(jnp.int32, (total, total), 1)
    source = (lax.rem(row, span) // small) * own + (row // span) * small + lax.rem(row, small)
    order = (source == col).astype(F32).astype(BF16)
    tok_p = jnp.dot(order, tok_all[...], preferred_element_type=F32).T
    meta_p = jnp.dot(order, meta_all[...], preferred_element_type=F32).T
    gate_p = meta_p[top : 2 * top] + meta_p[2 * top : 3 * top] + meta_p[3 * top : 4 * top]
    for g in range(groups):
        lo, hi = g * span, (g + 1) * span
        for c in range(copies):
            tok_t[g, :, c * span : (c + 1) * span] = tok_p[:, lo:hi]
            for chunk in range(per):
                k, at = chunk * copies + c, g * per + chunk
                id_row[at : at + 1, c * span : (c + 1) * span] = meta_p[k : k + 1, lo:hi]
                gate_row[at : at + 1, c * span : (c + 1) * span] = gate_p[k : k + 1, lo:hi]

    lanes = lax.broadcasted_iota(jnp.int32, (experts, total), 0).astype(F32)

    def mask_of(k):
        return id_row[pl.ds(k, 1), :] == lanes

    def partner(s):
        bit = 1 << s
        return me + bit * (1 - 2 * lax.rem(me // bit, 2))

    def h_copy(k, s):
        return remote(hs[s].at[k], hr[s].at[k], h_ssem.at[s, k], h_rsem.at[s, k], partner(s))

    def o_copy(q, s):
        return remote(os_[s].at[q], or_[s].at[q], o_ssem.at[s, q], o_rsem.at[s, q], partner(s))

    def h_rows(k, j, part):
        return h_ref[k, pl.ds(pl.multiple_of(part * half + j * fl, 16), fl), :]

    def h_sum(k, j, s, part):
        total_ = h_rows(k, j, part)
        for prior in range(s):
            total_ += hr[prior][k, j // (2 << prior), pl.ds(part * fl, fl), :].astype(F32)
        return total_

    def product(k):
        mask = mask_of(k)

        @pl.loop(0, depth // 8)
        def _(block):
            for inner in range(8):
                d = block * 8 + inner
                row = jnp.where(mask, tok_t[k // per, pl.ds(d, 1), :], 0.0)
                x_ref[pl.ds(pl.multiple_of(d * experts, experts), experts), :] = row.astype(BF16)

        h_ref[k] = jnp.dot(wt_ref[...], x_ref[...], preferred_element_type=F32)

    def h_send(k, s):
        if s > 0:
            h_copy(k, s - 1).wait_recv()
        bit = 1 << s
        base = (1 - lax.rem(me // bit, 2)) * bit + lax.rem(me, bit)
        for m in range(n // (2 * bit)):
            j = m * 2 * bit + base
            for part in range(2):
                hs[s][k, m, pl.ds(part * fl, fl), :] = h_sum(k, j, s, part).astype(hs[s].dtype)
        h_copy(k, s).start()

    def h_final(k):
        h_copy(k, bits - 1).wait_recv()
        gate = h_sum(k, me, bits, 0)
        act = gate / (1.0 + jnp.exp(-gate)) * h_sum(k, me, bits, 1)
        act_ref[...] = act * gate_row[pl.ds(k, 1), :]
        mask = mask_of(k)

        @pl.loop(0, fl // 8)
        def _(block):
            for inner in range(8):
                f = block * 8 + inner
                rows = pl.ds(pl.multiple_of(f * experts, experts), experts)
                placed = jnp.where(mask, act_ref[pl.ds(f, 1), :], 0.0)
                for c in range(copies):
                    a_ref[k // per, rows, :] += placed[:, c * span : (c + 1) * span]

    def o_sum(g, j, s):
        total_ = o_ref[g, pl.ds(pl.multiple_of(j * small, small), small), :]
        for prior in range(s):
            total_ += or_[prior][g, j // (2 << prior)].astype(F32)
        return total_

    def o_product(g):
        a_t = a_ref[g].T.astype(BF16)
        wide = width // 4

        @pl.loop(0, 4)
        def _(c):
            cols = pl.ds(pl.multiple_of(c * wide, wide), wide)
            o_ref[g, :, cols] = jnp.dot(a_t, d_ref[:, cols], preferred_element_type=F32)

    def o_send(g, s):
        if s > 0:
            o_copy(g, s - 1).wait_recv()
        bit = 1 << s
        base = (1 - lax.rem(me // bit, 2)) * bit + lax.rem(me, bit)
        for m in range(n // (2 * bit)):
            os_[s][g, m] = o_sum(g, m * 2 * bit + base, s).astype(os_[s].dtype)
        o_copy(g, s).start()

    def o_final(g):
        o_copy(g, bits - 1).wait_recv()
        out32[pl.ds(pl.multiple_of(g * small, small), small), :] = o_sum(g, me, bits)

    lags = [s + (s > 1) for s in range(bits + 1)]
    late = lags[bits]
    lead = per - 1 + late

    @pl.loop(0, (groups - 1) * per + lead + late + 1)
    def _(step):
        @pl.when(step < chunks)
        def _():
            product(step)
            h_send(step, 0)

        for s in range(1, bits):
            @pl.when((step >= lags[s]) & (step < chunks + lags[s]))
            def _():
                h_send(step - lags[s], s)

        @pl.when((step >= late) & (step < chunks + late))
        def _():
            h_final(step - late)

        for s in range(bits + 1):
            since = step - lead - lags[s]

            @pl.when((since >= 0) & (lax.rem(since + per * (late + chunks), per) == 0) & (since < chunks))
            def _():
                g = since // per
                if s == 0:
                    o_product(g)
                if s < bits:
                    o_send(g, s)
                else:
                    o_final(g)

        @pl.when(step == 1)
        def _():
            for i in range(1, n):
                scale_copy(i).start()

    out_ref[...] = out32[...].astype(BF16)
    for i in range(1, n):
        scale_copy(i).wait_recv()
    best = s_recv[0]
    for i in range(1, n):
        best = jnp.maximum(best, s_recv[i])
    scale_ref[:, pl.ds(0, 2 * half)] = best[:, : 2 * half] * root_d
    scale_ref[:, pl.ds(2 * half, width)] = best[:, 2 * half :] * root_f
    for i in range(1, n):
        meta_copy(i).wait_send()
        tok_copy(i).wait_send()
        scale_copy(i).wait_send()

    @pl.loop(0, chunks)
    def _(k):
        for s in range(bits):
            h_copy(k, s).wait_send()

    for g in range(groups):
        for s in range(bits):
            o_copy(g, s).wait_send()


def fused(tokens, gate_up, down_proj, expert_ids, gate_weights, owner_slot):
    n = lax.axis_size("ep")
    bits = n.bit_length() - 1
    own, width = tokens.shape
    depth, experts, both = gate_up.shape
    fl = down_proj.shape[0]
    top = expert_ids.shape[1]
    total = own * n
    groups = 2
    chunks = top
    span = total // groups
    vmem = pl.BlockSpec(memory_space=pltpu.VMEM)
    hbm = pl.BlockSpec(memory_space=pl.ANY)
    counts = [n >> (s + 1) for s in range(bits)]
    kinds = [BF16 if s else F32 for s in range(bits)]
    hidden_bufs = [pltpu.VMEM((chunks, c, 2 * fl, total), t) for c, t in zip(counts, kinds)]
    out_bufs = [pltpu.VMEM((groups, c, own // groups, width), t) for c, t in zip(counts, kinds)]
    return pl.pallas_call(
        functools.partial(fused_kernel, (n, bits, chunks, groups)),
        out_shape=(
            jax.ShapeDtypeStruct((own, width), BF16),
            jax.ShapeDtypeStruct((1, both + width), F32),
        ),
        in_specs=[vmem, vmem, vmem, vmem, hbm, hbm],
        out_specs=(vmem, vmem),
        scratch_shapes=[
            pltpu.VMEM((depth * experts, both), BF16),
            pltpu.VMEM((both, depth * experts), BF16),
            pltpu.VMEM((fl * experts, width), BF16),
            pltpu.VMEM((own, 128), F32),
            pltpu.VMEM((own, 128), BF16),
            pltpu.VMEM((total, depth), BF16),
            pltpu.VMEM((groups, depth, total), F32),
            pltpu.VMEM((total, 128), BF16),
            pltpu.VMEM((chunks, total), F32),
            pltpu.VMEM((chunks, total), F32),
            pltpu.VMEM((depth * experts, total), BF16),
            pltpu.VMEM((chunks, both, total), F32),
            pltpu.VMEM((fl, total), F32),
            pltpu.VMEM((groups, fl * experts, span), F32),
            pltpu.VMEM((groups, span, width), F32),
            pltpu.VMEM((own, width), F32),
            pltpu.VMEM((n, 1, both + width), F32),
            pltpu.VMEM((n, 1, both + width), F32),
            *hidden_bufs, *hidden_bufs, *out_bufs, *out_bufs,
            pltpu.SemaphoreType.DMA((2,)),
            pltpu.SemaphoreType.DMA((3, n)),
            pltpu.SemaphoreType.DMA((3, n)),
            pltpu.SemaphoreType.DMA((bits, chunks)),
            pltpu.SemaphoreType.DMA((bits, chunks)),
            pltpu.SemaphoreType.DMA((bits, groups)),
            pltpu.SemaphoreType.DMA((bits, groups)),
        ],
        compiler_params=pltpu.CompilerParams(
            collective_id=0, has_side_effects=True, vmem_limit_bytes=60 * 2**20
        ),
    )(
        tokens,
        expert_ids,
        gate_weights,
        owner_slot.reshape(1, experts),
        gate_up.reshape(depth * experts, both),
        down_proj.reshape(fl * experts, width),
    )


def layer(tokens, gate_up, down_proj, expert_ids, gate_weights, owner_slot):
    n = lax.axis_size("ep")
    own = tokens.shape[0]
    depth, experts, both = gate_up.shape
    partials = n * own * expert_ids.shape[1] * both
    aligned = (
        n & (n - 1) == 0 and depth % 128 == 0 and experts == n and experts % 16 == 0
        and down_proj.shape[0] % 16 == 0 and own % 16 == 0
    )
    args = (tokens, gate_up, down_proj, expert_ids, gate_weights, owner_slot)
    return fused(*args) if aligned and partials <= gate_up.size else shards(*args)


def solution(mesh):
    in_specs = (
        P(("parts", "ep"), None),
        P(("parts", "ep"), None, None),
        P(("parts", "ep"), None, None),
        P(("parts", "ep"), None),
        P(("parts", "ep"), None),
        P("parts"),
    )
    out_specs = (P(("parts", "ep"), None), P(("parts", "ep"), None))
    return jax.shard_map(layer, mesh=mesh, in_specs=in_specs, out_specs=out_specs, check_vma=False)
```
